8 devices in a mesh: rep: 1 (over z), dp: 8 (over x, y, core).
Axes of the slice: x: 2, y: 2, z: 1, core: 2. Of those that a mesh axis runs over, the one named last changes fastest.
Arguments:
- g_w_gate: bfloat16 [8, 2, 1024, 3328], P(('rep', 'dp'))
- g_w_up: bfloat16 [8, 2, 1024, 3328], P(('rep', 'dp'))
- g_w_down: bfloat16 [8, 2, 3328, 1024], P(('rep', 'dp'))
- w_gate: bfloat16 [2, 1024, 3328], replicated
- w_up: bfloat16 [2, 1024, 3328], replicated
- w_down: bfloat16 [2, 3328, 1024], replicated
- m_w_gate: float32 [2, 1024, 3328], P(None, 'dp')
- m_w_up: float32 [2, 1024, 3328], P(None, 'dp')
- m_w_down: float32 [2, 3328, 1024], P(None, 'dp')
- v_w_gate: float32 [2, 1024, 3328], P(None, 'dp')
- v_w_up: float32 [2, 1024, 3328], P(None, 'dp')
- v_w_down: float32 [2, 3328, 1024], P(None, 'dp')
Outputs:
- output 1: bfloat16 [2, 1024, 3328], P('rep')
- output 2: bfloat16 [2, 1024, 3328], P('rep')
- output 3: bfloat16 [2, 3328, 1024], P('rep')
- output 4: float32 [2, 1024, 3328], P('rep', 'dp')
- output 5: float32 [2, 1024, 3328], P('rep', 'dp')
- output 6: float32 [2, 3328, 1024], P('rep', 'dp')
- output 7: float32 [2, 1024, 3328], P('rep', 'dp')
- output 8: float32 [2, 1024, 3328], P('rep', 'dp')
- output 9: float32 [2, 3328, 1024], P('rep', 'dp')
All inputs are finite; a program needn't handle non-finite values.
Results may differ from the reference program's by a relative error of at most 0.022.
Values are sent between devices in bfloat16 or wider.
A program may use at most 2 GiB of HBM per device.

```python
import jax
import jax.numpy as jnp
from jax import lax

DEVICES = 8
D = 1024
FF = 3328
LAYERS = 2
NAMES = ("w_gate", "w_up", "w_down")
SHAPES = {"w_gate": (LAYERS, D, FF), "w_up": (LAYERS, D, FF), "w_down": (LAYERS, FF, D)}


def setup_inputs(seed: int = 0, part: int = 0) -> dict:
    kz, *keys = jax.random.split(jax.random.key(seed), 1 + 5 * len(NAMES))
    loud = 2.0 ** jax.random.uniform(kz, (), jnp.float32, -1.0, 1.0)
    drawn = {}
    for name, key, both in zip(NAMES, keys[:3], keys[3:6], strict=True):
        own = jax.random.normal(jax.random.fold_in(key, part), (DEVICES, *SHAPES[name]), jnp.float32)
        shared = jax.random.normal(jax.random.fold_in(both, part), SHAPES[name], jnp.float32)
        drawn["g_" + name] = (loud * (0.7 * shared / DEVICES + 0.7 * own * DEVICES**-0.5)).astype(jnp.bfloat16)
    for name, key in zip(NAMES, keys[6:9], strict=True):
        drawn[name] = (jax.random.normal(key, SHAPES[name], jnp.float32) * SHAPES[name][1] ** -0.5).astype(jnp.bfloat16)
    for name, key in zip(NAMES, keys[9:12], strict=True):
        drawn["m_" + name] = loud * 0.5 * jax.random.normal(key, SHAPES[name], jnp.float32)
    for name, key in zip(NAMES, keys[12:15], strict=True):
        drawn["v_" + name] = loud * loud * jax.random.uniform(key, SHAPES[name], jnp.float32, 0.5, 1.5)
    return drawn


def adamw(w, m, v, g):
    m = 0.9 * m + 0.1 * g
    v = 0.95 * v + 0.05 * g * g
    step = m * lax.rsqrt(v + 1e-8) + 0.1 * w
    return (w - 0.02 * step).astype(jnp.bfloat16), m, v


def clipped(gradients, sum_of_squares, count):
    factor = jnp.minimum(1.0, 0.5 * lax.rsqrt(sum_of_squares / count + 1e-30))
    return [g * factor for g in gradients]


def reference(g_w_gate, g_w_up, g_w_down, w_gate, w_up, w_down, m_w_gate, m_w_up, m_w_down, v_w_gate, v_w_up, v_w_down):
    def total(terms):
        return lax.scan(lambda so_far, term: (so_far + term.astype(jnp.float32), None), jnp.zeros(terms.shape[1:], jnp.float32), terms)[0]

    gradients = [total(terms).astype(jnp.bfloat16).astype(jnp.float32) for terms in (g_w_gate, g_w_up, g_w_down)]
    gradients = clipped(gradients, sum(jnp.sum(g * g) for g in gradients), sum(g.size for g in gradients))
    new = [
        adamw(w.astype(jnp.float32), m, v, g)
        for w, m, v, g in zip((w_gate, w_up, w_down), (m_w_gate, m_w_up, m_w_down), (v_w_gate, v_w_up, v_w_down), gradients, strict=True)
    ]
    return tuple(one[which] for which in range(3) for one in new)
```

```python
import functools

import jax
import jax.numpy as jnp
from jax import lax
from jax.experimental import pallas as pl
from jax.experimental.pallas import tpu as pltpu
from jax.sharding import PartitionSpec as P

MESH = pl.DeviceIdType.MESH
DIAGONAL, FIRST, SECOND, OWN = range(4)
FLIPS = (((1, 1), (1, 0), (0, 1), (0, 0)), ((1, 1), (0, 1), (1, 0), (0, 0)))
LAYERS = 2
SPLIT = 2


def flipped(fx, fy, fc):
    me = lax.axis_index("dp")
    x, y, c = me // 4, (me // 2) % 2, me % 2
    return (1 - x if fx else x) * 4 + (1 - y if fy else y) * 2 + (1 - c if fc else c)


def scatter_kernel(count, *refs):
    g, out, factor_ref = refs[:3], refs[3:6], refs[6]
    own, par, r1, r2 = refs[7:10], refs[10:13], refs[13:16], refs[16:19]
    squares, own_sem, psend_sem, precv_sem, send_sem, r1_sem, r2_sem, out_sem, ssend_sem, srecv_sem = refs[19:]
    me = lax.axis_index("dp")
    pieces = [(w, s, layer) for w in range(3) for s in range(SPLIT) for layer in range(LAYERS)]

    def rows(w):
        return own[w].shape[2] // SPLIT

    def span(w, s):
        return pl.ds(s * rows(w), rows(w))

    def source(w, layer, s, device):
        return g[w].at[0, layer, pl.ds(pl.multiple_of(device * (rows(w) * SPLIT) + s * rows(w), 16), rows(w))]

    def load(w, layer, whose, s):
        return pltpu.make_async_copy(
            source(w, layer, s, flipped(*FLIPS[layer][whose], 0)), own[w].at[layer, whose, span(w, s)], own_sem.at[w, layer, whose, s]
        )

    def swap(w, layer, whose, s):
        return pltpu.make_async_remote_copy(
            source(w, layer, s, flipped(*FLIPS[layer][whose], 1)),
            par[w].at[layer, whose, span(w, s)],
            psend_sem.at[w, layer, whose, s],
            precv_sem.at[w, layer, whose, s],
            device_id={"dp": flipped(0, 0, 1)},
            device_id_type=MESH,
        )

    def send(w, layer, whose, s):
        src = own[w].at[layer, whose, span(w, s)]
        if whose == SECOND:
            dst, sem, link = r2[w].at[layer, span(w, s)], r2_sem.at[w, layer, s], SECOND
        else:
            slot = 0 if whose == DIAGONAL else 1
            dst, sem, link = r1[w].at[layer, slot, span(w, s)], r1_sem.at[w, layer, slot, s], FIRST
        return pltpu.make_async_remote_copy(
            src, dst, send_sem.at[w, layer, whose, s], sem, device_id={"dp": flipped(*FLIPS[layer][link], 0)}, device_id_type=MESH
        )

    def result(w, layer, s):
        return pltpu.make_async_copy(own[w].at[layer, OWN, span(w, s)], out[w].at[layer, span(w, s)], out_sem.at[w, layer, s])

    def add(w, layer, whose, s, squares_so_far=None):
        columns = own[w].shape[3]
        width = columns // 2
        others = [par[w].at[layer, whose]]
        if whose == SECOND:
            others.append(r1[w].at[layer, 0])
        if whose == OWN:
            others += [r1[w].at[layer, 1], r2[w].at[layer]]
        mine = own[w].at[layer, whose]

        def body(i, so_far):
            at = pl.ds(pl.multiple_of(s * rows(w) + i * 16, 16), 16)
            for half in range(2):
                cut = pl.ds(half * width, width)
                total = mine[at, cut].astype(jnp.float32)
                for other in others:
                    total += other[at, cut].astype(jnp.float32)
                rounded = total.astype(jnp.bfloat16)
                mine[at, cut] = rounded
                if so_far is not None:
                    wide = rounded.astype(jnp.float32)
                    wide = wide * wide
                    for k in range(width // 128):
                        so_far = so_far + wide[:, k * 128 : (k + 1) * 128]
            return so_far

        return lax.fori_loop(0, rows(w) // 16, body, squares_so_far)

    for w, s, layer in pieces:
        load(w, layer, DIAGONAL, s).start()
    barrier = pltpu.get_barrier_semaphore()
    for other in range(1, 8):
        pl.semaphore_signal(barrier, inc=1, device_id={"dp": flipped(other // 4, (other // 2) % 2, other % 2)}, device_id_type=MESH)
    pl.semaphore_wait(barrier, 7)
    for whose in range(4):
        for w, s, layer in pieces:
            if whose != DIAGONAL:
                load(w, layer, whose, s).start()
            swap(w, layer, whose, s).start()

    so_far = jnp.zeros((16, 128), jnp.float32)
    for whose in range(4):
        for w, s, layer in pieces:
            load(w, layer, whose, s).wait()
            swap(w, layer, whose, s).wait_recv()
            if whose == SECOND:
                send(w, layer, DIAGONAL, s).wait_recv()
            if whose == OWN:
                send(w, layer, FIRST, s).wait_recv()
                send(w, layer, SECOND, s).wait_recv()
                so_far = add(w, layer, whose, s, so_far)
                result(w, layer, s).start()
            else:
                add(w, layer, whose, s)
                send(w, layer, whose, s).start()

    squares[me] = so_far[:8] + so_far[8:]

    def tell(other):
        return pltpu.make_async_remote_copy(
            squares.at[me],
            squares.at[me],
            ssend_sem.at[other],
            srecv_sem.at[other],
            device_id={"dp": flipped(other // 4, (other // 2) % 2, other % 2)},
            device_id_type=MESH,
        )

    for other in range(1, 8):
        tell(other).start()
    for other in range(1, 8):
        tell(other).wait_recv()
    total = squares[0]
    for device in range(1, 8):
        total = total + squares[device]
    total = jnp.sum(jnp.sum(total, axis=1, keepdims=True), axis=0, keepdims=True)
    factor = jnp.minimum(1.0, 0.5 * lax.rsqrt(total / count + 1e-30))
    factor_ref[...] = jnp.broadcast_to(factor, factor_ref.shape)

    for other in range(1, 8):
        tell(other).wait_send()
    for w, s, layer in pieces:
        result(w, layer, s).wait()
        for whose in range(4):
            swap(w, layer, whose, s).wait_send()
            if whose != OWN:
                send(w, layer, whose, s).wait_send()


def scatter(terms, blocks, count):
    shapes = [b.shape[1:] for b in blocks]

    def buffers(*lead):
        return [pltpu.VMEM((LAYERS, *lead, *shape), jnp.bfloat16) for shape in shapes]

    dma = pltpu.SemaphoreType.DMA
    any_space = pl.BlockSpec(memory_space=pl.ANY)
    return pl.pallas_call(
        functools.partial(scatter_kernel, count),
        name="scatter",
        out_shape=[jax.ShapeDtypeStruct(b.shape, jnp.bfloat16) for b in blocks] + [jax.ShapeDtypeStruct((8, 128), jnp.float32)],
        in_specs=[any_space] * 3,
        out_specs=[any_space] * 3 + [pl.BlockSpec(memory_space=pltpu.VMEM)],
        scratch_shapes=[
            *buffers(4),
            *buffers(4),
            *buffers(2),
            *buffers(),
            pltpu.VMEM((8, 8, 128), jnp.float32),
            dma((3, LAYERS, 4, SPLIT)),
            dma((3, LAYERS, 4, SPLIT)),
            dma((3, LAYERS, 4, SPLIT)),
            dma((3, LAYERS, 3, SPLIT)),
            dma((3, LAYERS, 2, SPLIT)),
            dma((3, LAYERS, SPLIT)),
            dma((3, LAYERS, SPLIT)),
            dma((8,)),
            dma((8,)),
        ],
        compiler_params=pltpu.CompilerParams(collective_id=0, has_side_effects=True, vmem_limit_bytes=60 * 1024 * 1024),
    )(*terms)


def adamw_kernel(me_ref, factor_ref, g_ref, w_ref, m_ref, v_ref, first_ref, second_ref, new_m_ref, new_v_ref):
    factor = factor_ref[0:1, 0:1]
    for layer, new_w_ref in enumerate((first_ref, second_ref)):
        g = g_ref[layer].astype(jnp.float32) * factor
        m = 0.9 * m_ref[layer] + 0.1 * g
        v = 0.95 * v_ref[layer] + 0.05 * g * g
        w = w_ref[layer].astype(jnp.float32)
        step = m * lax.rsqrt(v + 1e-8) + 0.1 * w
        new_w_ref[...] = (w - 0.02 * step).astype(jnp.bfloat16)
        new_m_ref[layer] = m
        new_v_ref[layer] = v


def adamw(me, factor, g, w, m, v):
    _, rows, columns = m.shape
    steps = 4
    cut = rows // steps
    block = pl.BlockSpec((LAYERS, cut, columns), lambda i, me: (0, i, 0))
    flat = pl.BlockSpec((cut, columns), lambda i, me: (i, 0))
    return pl.pallas_call(
        adamw_kernel,
        name="adamw",
        out_shape=[jax.ShapeDtypeStruct((rows, columns), jnp.bfloat16)] * 2 + [jax.ShapeDtypeStruct(m.shape, jnp.float32)] * 2,
        grid_spec=pltpu.PrefetchScalarGridSpec(
            num_scalar_prefetch=1,
            grid=(steps,),
            in_specs=[
                pl.BlockSpec((8, 128), lambda i, me: (0, 0)),
                block,
                pl.BlockSpec((LAYERS, cut, columns), lambda i, me: (0, me[0] * steps + i, 0)),
                block,
                block,
            ],
            out_specs=[flat, flat, block, block],
        ),
        compiler_params=pltpu.CompilerParams(vmem_limit_bytes=40 * 2**20),
        cost_estimate=pl.CostEstimate(flops=20 * m.size * 100, bytes_accessed=22 * m.size, transcendentals=m.size),
    )(me, factor, g, w, m, v)


def join(where, layer, pieces, shape, so_far):
    rows, columns = pieces[0].shape
    n = len(pieces)
    extra = [] if so_far is None else [so_far]

    def kernel(where_ref, *refs):
        parts = refs[:n]
        out, held, in_sem, out_sem = refs[-4:]

        def take(k):
            return pltpu.make_async_copy(parts[k], held.at[k], in_sem.at[k])

        def put(k):
            at = pl.ds(pl.multiple_of(where_ref[k] * rows, 16), rows)
            return pltpu.make_async_copy(held.at[k], out.at[layer, at], out_sem.at[k])

        for k in range(n):
            take(k).start()
        for k in range(n):
            take(k).wait()
            put(k).start()
        for k in range(n):
            put(k).wait()

    any_space = pl.BlockSpec(memory_space=pl.ANY)
    return pl.pallas_call(
        kernel,
        name="join",
        out_shape=jax.ShapeDtypeStruct(shape, jnp.bfloat16),
        in_specs=[pl.BlockSpec(memory_space=pltpu.SMEM)] + [any_space] * (n + len(extra)),
        out_specs=any_space,
        scratch_shapes=[pltpu.VMEM((n, rows, columns), jnp.bfloat16), pltpu.SemaphoreType.DMA((n,)), pltpu.SemaphoreType.DMA((n,))],
        input_output_aliases={n + 1: 0} if extra else {},
        compiler_params=pltpu.CompilerParams(vmem_limit_bytes=20 * 2**20),
        cost_estimate=pl.CostEstimate(flops=100 * n * rows * columns, bytes_accessed=4 * n * rows * columns, transcendentals=0),
    )(where, *pieces, *extra)


def solution(mesh):
    def step(*arrays):
        terms, weights, m, v = (arrays[i : i + 3] for i in (0, 3, 6, 9))
        count = float(sum(w.size for w in weights))
        *gradients, factor = scatter(terms, m, count)
        me = lax.axis_index("dp")
        me_array = jnp.full((1,), me, jnp.int32)

        def hop(array, fx, fy, fc):
            return lax.ppermute(array, "dp", [(d, d ^ (4 * fx + 2 * fy + fc)) for d in range(8)])

        new = [adamw(me_array, factor, *one) for one in zip(gradients, weights, m, v, strict=True)]
        whole = []
        for i, (first, second, *_) in enumerate(new):
            result = None
            for layer, mine in enumerate((first, second)):
                near = FLIPS[layer][FIRST], FLIPS[layer][SECOND]
                one = hop(mine, *near[0], 0)
                two = hop(mine, *near[1], 0)
                both = hop(one, *near[1], 0)
                here = [mine, one, two, both]
                there = [hop(a, 0, 0, 1) for a in here]
                flips = [(0, 0), near[0], near[1], (1, 1)]
                where = jnp.stack([flipped(*f, fc) for fc in (0, 1) for f in flips]).astype(jnp.int32)
                result = join(where, layer, here + there, weights[i].shape, result)
            whole.append(result)
        return (*whole, *(one[2] for one in new), *(one[3] for one in new))

    all_of, cut = P(None, None, None), P(None, "dp", None)
    return jax.shard_map(
        step,
        mesh=mesh,
        in_specs=(P(("rep", "dp"), None, None, None),) * 3 + (all_of,) * 3 + (cut,) * 6,
        out_specs=(P("rep", None, None),) * 3 + (P("rep", "dp", None),) * 6,
        check_vma=False,
    )
```
